256 devices in a mesh: space: 256 (over x, z, y, core).
Axes of the slice: x: 4, y: 4, z: 8, core: 2. Of those that a mesh axis runs over, the one named last changes fastest.
Arguments:
- coords: float32 [4096, 3, 128], P('space'), may hold values from -3 to 3
- force: float32 [4096, 3, 128], P('space'), may hold values from -12 to 12
- restraint: float32 [4096, 128], P('space'), may hold values from 0.25 to 4
- neighbors: int32 [4096, 32], P('space'), may hold values from 0 to 4095, as said below
- mask: int32 [4096, 32], P('space'), may hold values from 0 to 1, as said below
Outputs:
- solution_field: float32 [4096, 3, 128], P('space')
- residual: float32 [4096, 3, 128], P('space')
The draws below stay inside these ranges and needn't reach their ends.
Inputs may be any that keep to these rules, and one draw needn't show every extreme that they name: `neighbors`: for every block b, the live entries name distinct blocks c with |c - b| <= 15; b itself is always live; if b lists c live then c lists b live; entries with mask 0 name b itself. `mask`: marks the live entries of neighbors.
All inputs are finite; a program needn't handle non-finite values.
Results may differ from the reference program's by a relative error of at most 0.0003.
Values sent between devices are 32-bit elements; how exact they have to be, the bound alone decides.
A program may use at most 64 MiB of HBM per device.

```python
import math
import jax
import jax.numpy as jnp
from jax import lax

BA = 128
NB = 32
BLK_DEV = 16
ITERS = 2
NBLK = 4096


def neighbor_tables(key):
    window = min(BLK_DEV, (NB - 1) // 2)
    block_ids = jnp.arange(NBLK, dtype=jnp.int32)
    offsets = jnp.arange(2 * window + 1, dtype=jnp.int32) - window
    partner = block_ids[:, None] + offsets[None, :]
    inside = (partner >= 0) & (partner < NBLK)
    lower_id = jnp.clip(jnp.minimum(partner, block_ids[:, None]), 0, NBLK - 1)
    upper_id = jnp.clip(jnp.maximum(partner, block_ids[:, None]), 0, NBLK - 1)
    pair_code = lower_id * NBLK + upper_id
    link_key = jax.random.fold_in(key, 11)
    hashed = jax.vmap(jax.vmap(lambda code: jax.random.randint(jax.random.fold_in(link_key, code), (), 0, 5)))(pair_code)
    linked = inside & ((hashed < 4) | (partner == block_ids[:, None]))
    padding = NB - (2 * window + 1)
    partner_full = jnp.concatenate([partner, jnp.broadcast_to(block_ids[:, None], (NBLK, padding))], axis=1)
    linked_full = jnp.concatenate([linked, jnp.zeros((NBLK, padding), dtype=bool)], axis=1)
    scores = jax.random.randint(jax.random.fold_in(key, 12), (NBLK, NB), 0, 2 ** 20) * NB + jnp.arange(NB, dtype=jnp.int32)[None, :]
    ranking = jnp.argsort(scores, axis=1)
    partner_full = jnp.take_along_axis(partner_full, ranking, axis=1)
    linked_full = jnp.take_along_axis(linked_full, ranking, axis=1)
    chosen = jnp.where(linked_full, partner_full, block_ids[:, None]).astype(jnp.int32)
    return (chosen, linked_full.astype(jnp.int32))


def draw_neighbors(key, part):
    return neighbor_tables(key)[0]


def draw_mask(key, part):
    return neighbor_tables(key)[1]


def draw_force(key, part):
    rising = 3.0 ** (0.5 * jnp.arange(NBLK, dtype=jnp.float32) / (NBLK - 1))
    normal_part = jnp.clip(jax.random.normal(jax.random.fold_in(key, 23), (NBLK, 3, BA), jnp.float32), -4.0, 4.0)
    values = normal_part * rising[:, None, None]
    return values.astype(jnp.float32)


def steps_of(rng, dims, pieces, smallest, high):
    loudness, own = 1.0, jax.random.fold_in(rng, 6)
    for dim, blocks in pieces:
        steps = jnp.exp(jax.random.uniform(jax.random.fold_in(own, dim), (blocks,), jnp.float32, smallest / len(pieces), high / len(pieces)))
        loudness = loudness * jnp.repeat(steps, dims[dim] // blocks).reshape([-1 if axis == dim else 1 for axis in range(len(dims))])
    return loudness


def noise(own_key, shape, spread, bound, split=(), held_as=jnp.bfloat16):
    array = spread * jax.random.normal(own_key, shape, jnp.float32)
    if split:
        array = array * steps_of(own_key, shape, split, -0.22, 0.18)
    return jnp.clip(array, -bound, bound).astype(held_as)


def setup_inputs(seed: int = 0) -> dict:
    key_of = jax.random.split(jax.random.key(seed), 6)
    return {
        "coords": noise(key_of[0], (NBLK, 3, BA), 0.5, 3.0, ((0, 256),), jnp.float32),
        "force": draw_force(jax.random.fold_in(key_of[5], 71), 0),
        "restraint": jnp.clip(jnp.exp(math.log(4.0) - 2.7725887 * jax.random.uniform(key_of[2], (NBLK, BA), jnp.float32) ** steps_of(key_of[2], (NBLK, BA), ((0, 256),), -0.2, 0.2)), 0.25, 4.0),
        "neighbors": draw_neighbors(jax.random.fold_in(key_of[5], 71), 0),
        "mask": draw_mask(jax.random.fold_in(key_of[5], 71), 0),
    }


def block_product(own_coords, own_values, own_spring, far_coords, far_values, live_flags):
    offset = far_coords[:, :, None, :] - own_coords[None, :, :, None]
    squared = jnp.sum(offset * offset, axis=1)
    soften = 1.0 + squared
    weight = live_flags[:, None, None] / (own_coords.shape[-1] * soften * soften)
    motion = jnp.sum(offset * (own_values[None, :, :, None] - far_values[:, :, None, :]), axis=1)
    strength = weight * motion
    pulled = jnp.sum(strength[:, None, :, :] * offset, axis=(0, 3))
    return own_spring[None, :] * own_values + pulled


def apply_operator(vector, coords, restraint, neighbors, live_mask):
    def one_block(packed):
        own_coords, own_values, own_spring, near_rows, live_flags = packed
        near_rows = near_rows.astype(jnp.int32)
        return block_product(own_coords, own_values, own_spring, coords[near_rows], vector[near_rows], live_flags)

    return lax.map(one_block, (coords, vector, restraint, neighbors, live_mask))


def reference(coords, force, restraint, neighbors, mask):
    live_mask = mask.astype(jnp.float32)
    solution = jnp.zeros_like(force)
    residual = force
    direction = force
    norm_now = jnp.sum(residual * residual)
    for iteration in range(ITERS):
        image = apply_operator(direction, coords, restraint, neighbors, live_mask)
        step_size = norm_now / jnp.sum(direction * image)
        solution = solution + step_size * direction
        residual = residual - step_size * image
        if iteration + 1 < ITERS:
            norm_next = jnp.sum(residual * residual)
            direction = residual + (norm_next / norm_now) * direction
            norm_now = norm_next
    return solution, residual
```

```python
import functools

import jax
import jax.numpy as jnp
from jax import lax
from jax.experimental import pallas as pl
from jax.experimental.pallas import tpu as pltpu
from jax.sharding import PartitionSpec as P

AXIS = "space"
MESH = pl.DeviceIdType.MESH
BLK = 16
BA = 128
NB = 32
PAIRS = BLK // 2
LAG = 2
LAG1 = LAG + 1
STAGES = 12
F32, BF16, F8 = jnp.float32, jnp.bfloat16, jnp.float8_e4m3fn
SHRINK = 2.0**-8
FAR = 1.5 * 2.0**63
SCALE = SHRINK * SHRINK / BA


def split2(value):
    high = value.astype(BF16).astype(F32)
    return high, value - high


def split3(value):
    high, rest = split2(value)
    middle, low = split2(rest)
    return high, middle, low


def body(
    x_acc, y_acc, z_acc, c_hbm, f_hbm, r_hbm, nb_hbm, mk_hbm, y_hbm, z_hbm, step0_ref, step1_ref, beta_ref,
    c_ref, f_ref, r_ref, nb_ref, mk_ref, in_sem, out_sem, zown,
    halo_c, halo_f, yown, yhalo, stage, enc, far_t, at, bm, feat, wh, wl, yacc, rows_v, rows_s, dmat,
    part, others, ready, c_send, c_recv, f_send, f_recv, y_send, y_recv, sum_send, sum_recv,
):
    me = lax.axis_index(AXIS)
    core, yy, zz, xx = me % 2, (me // 2) % 4, (me // 8) % 8, me // 64
    rank_a, rank_b = zz * 2 + core, xx * 4 + yy

    def member_a(rank):
        return xx * 64 + (rank // 2) * 8 + yy * 2 + rank % 2

    def member_b(rank):
        return (rank // 4) * 64 + zz * 8 + (rank % 4) * 2 + core

    before, after = (me + 255) % 256, (me + 1) % 256
    first, last = me == 0, me == 255

    pairs_in = ((c_hbm, c_ref), (f_hbm, f_ref), (r_hbm, r_ref), (nb_hbm, nb_ref), (mk_hbm, mk_ref))
    loads = [pltpu.make_async_copy(source, target, in_sem.at[k]) for k, (source, target) in enumerate(pairs_in)]
    for load in loads:
        load.start()

    barrier = pltpu.get_barrier_semaphore()
    for target in (before, after):
        pl.semaphore_signal(barrier, inc=1, device_id=(target,), device_id_type=MESH)
    for t in range(1, 16):
        pl.semaphore_signal(barrier, inc=1, device_id=(member_a((rank_a + t) % 16),), device_id_type=MESH)
        pl.semaphore_signal(barrier, inc=1, device_id=(member_b((rank_b + t) % 16),), device_id_type=MESH)

    for load in loads:
        load.wait()

    place = nb_ref[...] - me * BLK + BLK
    enc[...] = jnp.full((128, 128), -1.0, F32)
    enc[32 : 32 + BLK, 0:NB] = jnp.where(mk_ref[...] == 1, place, -1).astype(F32)
    slots = enc[...].T
    window = lax.broadcasted_iota(jnp.int32, (48, 128), 0).astype(F32)
    lane = lax.broadcasted_iota(jnp.int32, (48, 128), 1)
    hit = window == slots[0:1, :]
    for s in range(1, NB):
        hit = jnp.logical_or(hit, window == slots[s : s + 1, :])
    far_t[...] = jnp.where(jnp.logical_or(hit, jnp.logical_or(lane < 32, lane >= 32 + BLK)), 0.0, FAR)

    one = jnp.ones((BLK, BA), F32)

    turn = [0]

    def spread_rows(rows, stride):
        turn[0] = (turn[0] + 1) % STAGES
        target = stage.at[turn[0]]
        for k, row in enumerate(rows):
            target[pl.ds(k, BLK, stride=stride), :] = row
        return target

    def far_side(group, c):
        h, m, l = zip(*(split3(c[a]) for a in range(3)))
        norm = split3(c[0] * c[0] + c[1] * c[1] + c[2] * c[2])
        zero = jnp.zeros((BLK, BA), F32)
        rows = [*h, *h, *h, *m, *m, *l, *norm, one, one, one] + [zero] * 8
        source = spread_rows(rows, 32)

        def fill(e):
            block = group * BLK + e
            tall = jnp.concatenate([source[e * 32 : e * 32 + 32, :], jnp.zeros((96, BA), F32)], axis=0)
            at[block * BA : (block + 1) * BA, :] = (tall.T + far_t[block : block + 1, :]).astype(BF16)

        return fill

    def near_side(c):
        h, m, l = zip(*(split3(c[a]) for a in range(3)))
        norm = split3(1.0 + (c[0] * c[0] + c[1] * c[1] + c[2] * c[2]))
        zero = jnp.zeros((BLK, BA), F32)
        h, m, l = ([-2.0 * SHRINK * v for v in vs] for vs in (h, m, l))
        norm = [SHRINK * v for v in norm]
        shrink = jnp.full((BLK, BA), SHRINK, F32)
        rows = [*h, *m, *l, *h, *m, *h, shrink, shrink, shrink, *norm] + [zero] * 8
        source = spread_rows(rows, 32)
        row = lax.broadcasted_iota(jnp.int32, (96, BA), 0)
        for b in range(BLK):
            lanes = slice((b % 2) * BA, (b % 2 + 1) * BA)
            full = jnp.concatenate([source[b * 32 : b * 32 + 32, :], jnp.where(row == b, 1.0, 0.0)], axis=0)
            bm[b // 2, :, lanes] = full.astype(BF16)

    def store_features(group, values, high_row, low_row):
        highs, lows = zip(*(split2(v) for v in values))
        sources = [(spread_rows(split, 16), row) for split, row in ((highs, high_row), (lows, low_row))]

        def fill(e):
            lanes = slice((group * BLK + e) * BA, (group * BLK + e + 1) * BA)
            for source, row in sources:
                feat[row : row + 16, lanes] = source[e * 16 : e * 16 + 16, :].astype(BF16)

        return fill

    def field_features(group, c, v):
        p = c[0] * v[0] + c[1] * v[1] + c[2] * v[2]
        values = [c[a] * p for a in range(3)] + [p] + [v[b] for b in range(3)]
        values += [c[a] * v[b] for a in range(3) for b in range(3)]
        return store_features(group, values, 16, 0)

    def place_features(group, c):
        zero = jnp.zeros((BLK, BA), F32)
        values = [one, c[0], c[1], c[2], c[0] * c[0], c[1] * c[1], c[2] * c[2]]
        values += [c[0] * c[1], c[0] * c[2], c[1] * c[2]] + [zero] * 6
        return store_features(group, values, 32, 48)

    def fill_all(*fills):
        for e in range(BLK):
            for fill in fills:
                fill(e)

    def tiles_of(p, inside):
        if inside:
            return [((BLK + 2 * k, BLK + 2 * k + 1), k) for k in range(8)]
        low = [(e, e + 1) for e in range(2 * p + 2, BLK, 2)]
        up = [(e, e + 1) for e in range(2 * BLK, 2 * BLK + 2 * p, 2)]
        return [(blocks, 8 + k) for k, blocks in enumerate(low + up + [(2 * p + 1, 2 * BLK + 2 * p)])]

    def lanes_of(rows, blocks):
        i, j = blocks
        if j == i + 1:
            return feat[rows, i * BA : (j + 1) * BA]
        return jnp.concatenate([feat[rows, e * BA : (e + 1) * BA] for e in blocks], axis=1)

    zeros = jnp.zeros((BA, BA), BF16)
    register = [0, 0]

    def push(q, tile):
        register[q] = 1 - register[q]
        pltpu.matmul_push_rhs(tile, staging_register=register[q], mxu_index=q)
        return register[q]

    steps = [(pair, t) for pair in range(PAIRS // 2) for t in range(8)]

    def build(inside, ahead=None, collected=None):
        lists = [tiles_of(p, inside) for p in range(PAIRS)]

        def start(q, i):
            pair, t = steps[i]
            p = 2 * pair + q
            wide = jnp.concatenate([bm[p], jnp.zeros((BA, 2 * BA), BF16)], axis=0)
            staged = push(q, wide)
            for k, e in enumerate(lists[p][t][0]):
                lhs = jnp.concatenate([at[e * BA : (e + 1) * BA, :], zeros], axis=1)
                pltpu.matmul_acc_lhs(x_acc[q][i % LAG1][k], lhs, load_staged_rhs=staged if k == 0 else None)

        def finish(q, i):
            pair, t = steps[i]
            p = 2 * pair + q
            blocks, slot = lists[p][t]
            for k in range(2):
                x = pltpu.matmul_pop(x_acc[q][i % LAG1][k])
                w = 1.0 / (x * x)
                high = w.astype(BF16)
                low = (w - high.astype(F32)).astype(F8)
                rows = slice(slot * 2 * BA + k * BA, slot * 2 * BA + (k + 1) * BA)
                wh[p, rows, :] = high
                wl[p, rows, :] = low
            acc_h, acc_l = y_acc[q][pair % 2]
            tile = slice(slot * 2 * BA, (slot + 1) * 2 * BA)
            staged = push(q, wh[p, tile, :])
            pltpu.matmul_acc_lhs(acc_h, lanes_of(slice(0, 64), blocks), load_staged_rhs=staged)
            staged = push(q, wl[p, tile, :])
            pltpu.matmul_acc_lhs(acc_l, lanes_of(slice(16, 48), blocks), load_staged_rhs=staged)

        def collect(pair):
            for q in range(2):
                p = 2 * pair + q
                acc_h, acc_l = y_acc[q][pair % 2]
                total_h, total_l = pltpu.matmul_pop(acc_h), pltpu.matmul_pop(acc_l)
                if inside:
                    yacc[p, 0:64, :] = total_h
                    yacc[p, 64:96, :] = total_l
                    continue
                total_h += yacc[p, 0:64, :]
                total_l += yacc[p, 64:96, :]
                value = total_h[0:16] + total_h[16:32] + total_l[0:16]
                still = total_h[32:48] + total_h[48:64] + total_l[16:32]
                for k in range(2):
                    rows = slice((2 * p + k) * 16, (2 * p + k + 1) * 16)
                    rows_v[rows, :] = value[:, k * BA : (k + 1) * BA]
                    rows_s[rows, :] = still[:, k * BA : (k + 1) * BA]

        for i in range(len(steps) + LAG):
            if ahead is not None:
                ahead(i)
            for q in range(2):
                if i < len(steps):
                    start(q, i)
            for q in range(2):
                if i >= LAG:
                    finish(q, i - LAG)
            if i >= LAG + 9 and (i - LAG - 9) % 8 == 0:
                collect((i - LAG - 9) // 8)
                if collected is not None:
                    collected((i - LAG - 9) // 8)
        collect(PAIRS // 2 - 1)
        if collected is not None:
            collected(PAIRS // 2 - 1)

    def product(phase):
        lists = [tiles_of(p, phase == 0) for p in range(PAIRS)]
        if phase > 0:
            early = [[tile for tile in tiles if all(e % BLK < 8 for e in tile[0])] for tiles in lists]
            lists = early if phase == 1 else [
                [tile for tile in tiles if tile not in first] for tiles, first in zip(lists, early)
            ]

        def collect(pair):
            for q in range(2):
                p = 2 * pair + q
                acc_h, acc_l = z_acc[q][pair % 2]
                total_h, total_l = pltpu.matmul_pop(acc_h), pltpu.matmul_pop(acc_l)
                value = total_h[0:16] + total_h[16:32] + total_l
                if phase > 0:
                    value += yacc[p, 0:16, :]
                if phase < 2:
                    yacc[p, 0:16, :] = value
                    continue
                for k in range(2):
                    rows_v[(2 * p + k) * 16 : (2 * p + k + 1) * 16, :] = value[:, k * BA : (k + 1) * BA]

        count = len(lists[0])
        assert all(len(tiles) == count for tiles in lists)
        for i in range(PAIRS // 2 * count):
            pair, t = i // count, i % count
            for q in range(2):
                p = 2 * pair + q
                blocks, slot = lists[p][t]
                acc_h, acc_l = z_acc[q][pair % 2]
                rows = slice(slot * 2 * BA, (slot + 1) * 2 * BA)
                staged = push(q, wh[p, rows, :])
                pltpu.matmul_acc_lhs(acc_h, lanes_of(slice(0, 32), blocks), load_staged_rhs=staged)
                staged = push(q, wl[p, rows, :])
                pltpu.matmul_acc_lhs(acc_l, lanes_of(slice(16, 32), blocks), load_staged_rhs=staged)
            if i > count and i % count == 1:
                collect(i // count - 1)
        collect(PAIRS // 2 - 1)

    def combine(half, c, v):
        t = [rows_v[pl.ds(k + half * 128, 8, stride=16), :] for k in range(16)]
        cv = c[0] * t[4] + c[1] * t[5] + c[2] * t[6]
        out = []
        for a in range(3):
            gone = t[a] - c[a] * t[3] + c[a] * cv
            gone = gone - (c[0] * t[7 + 3 * a] + c[1] * t[8 + 3 * a] + c[2] * t[9 + 3 * a])
            kept = sum(dmat[half, PACK[a][b]] * v[b] for b in range(3))
            out.append(kept - gone * SCALE)
        return out

    c = [c_ref[a] for a in range(3)]
    f = [f_ref[a] for a in range(3)]
    near_side(c)
    fill_all(far_side(1, c), field_features(1, c, f), place_features(1, c))

    pl.semaphore_wait(barrier, 32)

    def exchange(source, target, send, recv):
        up, down = (
            pltpu.make_async_remote_copy(
                src_ref=source, dst_ref=target.at[k], send_sem=send.at[k], recv_sem=recv.at[k],
                device_id=(neighbour,), device_id_type=MESH,
            )
            for k, neighbour in ((0, after), (1, before))
        )

        @pl.when(jnp.logical_not(last))
        def _():
            up.start()

        @pl.when(jnp.logical_not(first))
        def _():
            down.start()

        @pl.when(first)
        def _():
            target[0] = jnp.zeros(target.shape[1:], F32)

        @pl.when(last)
        def _():
            target[1] = jnp.zeros(target.shape[1:], F32)

        def finish():
            @pl.when(jnp.logical_not(last))
            def _():
                up.wait_send()
                down.wait_recv()

            @pl.when(jnp.logical_not(first))
            def _():
                down.wait_send()
                up.wait_recv()

        return finish

    finish_c = exchange(c_ref, halo_c, c_send, c_recv)
    finish_f = exchange(f_ref, halo_f, f_send, f_recv)
    for t in range(1, 16):
        pl.semaphore_signal(ready, inc=1, device_id=(member_b((rank_b + t) % 16),), device_id_type=MESH)

    build(True)

    finish_c()
    finish_f()
    hc = [[halo_c[side, a] for a in range(3)] for side in range(2)]
    far_fill, field_fill = {}, {}

    def open_far(side):
        far_fill[side] = far_side(2 * side, hc[side])

    def open_fields(side):
        hf = [halo_f[side, a] for a in range(3)]
        fills = (field_features(2 * side, hc[side], hf), place_features(2 * side, hc[side]))
        field_fill[side] = lambda e: [fill(e) for fill in fills]

    def fill_blocks(fills, side, *blocks):
        for e in blocks:
            fills[side](e)

    def ahead(i):
        if i == 0:
            open_far(0)
            fill_blocks(far_fill, 0, 2, 3, 4, 5)
        if i == 1:
            fill_blocks(far_fill, 0, 6, 7)
            open_fields(0)
            fill_blocks(field_fill, 0, 2, 3, 4, 5)
        if i == 2:
            fill_blocks(far_fill, 0, 8, 9)
            fill_blocks(field_fill, 0, 6, 7)
            open_far(1)
        if i == 3:
            fill_blocks(far_fill, 0, 10, 11)
            fill_blocks(field_fill, 0, 8, 9)
            fill_blocks(far_fill, 1, 0, 1, 2)
        if i == 4:
            fill_blocks(far_fill, 0, 12, 13)
            fill_blocks(field_fill, 0, 10, 11)
            fill_blocks(far_fill, 1, 3, 4, 5, 6)
            open_fields(1)
        if i == 5:
            fill_blocks(far_fill, 0, 14, 15, 1)
            fill_blocks(field_fill, 0, 12, 13)
            fill_blocks(far_fill, 1, 7, 8, 9, 10)
            fill_blocks(field_fill, 1, 0, 1, 2, 3)
        if i == 6:
            fill_blocks(far_fill, 1, 11, 12, 13, 14)
            fill_blocks(field_fill, 0, 14, 15, 1)
            fill_blocks(field_fill, 1, 4, 5, 6, 7, 8)
        if i == 7:
            fill_blocks(field_fill, 1, 9, 10, 11, 12, 13, 14)

    finishes, copies_out = [], []

    def first_product(pair):
        if pair % 2 == 0:
            return
        half = pair // 2
        rows = slice(8 * half, 8 * half + 8)
        ch = [c_ref[a, rows] for a in range(3)]
        fh = [f_ref[a, rows] for a in range(3)]
        s = [rows_s[pl.ds(k + half * 128, 8, stride=16), :] for k in range(10)]
        for a, b, k in ((0, 0, 4), (1, 1, 5), (2, 2, 6), (0, 1, 7), (0, 2, 8), (1, 2, 9)):
            entry = (s[k] - ch[a] * s[1 + b] - ch[b] * s[1 + a] + ch[a] * ch[b] * s[0]) * SCALE
            dmat[half, PACK[a][b]] = entry + r_ref[rows] if a == b else entry
        value = combine(half, ch, fh)
        for a in range(3):
            yown[half, a] = value[a]
        finishes.append(exchange(yown.at[half], yhalo.at[half], y_send.at[half], y_recv.at[half]))
        copies_out.append(pltpu.make_async_copy(yown.at[half], y_hbm.at[:, rows], out_sem.at[half]))
        copies_out[-1].start()

    build(False, ahead, first_product)

    y = [jnp.concatenate([yown[0, a], yown[1, a]], axis=0) for a in range(3)]
    fill_all(field_features(1, c, y))
    product(0)
    for half in range(2):
        finishes[half]()
        for side in range(2):
            blank = jnp.zeros((8, BA), F32)
            parts = [[yhalo[half, side, a], blank] for a in range(3)]
            hy = [jnp.concatenate(part if half == 0 else part[::-1], axis=0) for part in parts]
            fill = field_features(2 * side, hc[side], hy)
            for e in range(8 * half, 8 * half + 8):
                fill(e)
        product(1 + half)
    halves = [
        combine(half, [c[a][8 * half : 8 * half + 8] for a in range(3)], [yown[half, a] for a in range(3)])
        for half in range(2)
    ]
    z = [jnp.concatenate([halves[0][a], halves[1][a]], axis=0) for a in range(3)]
    for a in range(3):
        zown[a] = z[a]
    z_out = pltpu.make_async_copy(zown, z_hbm, out_sem.at[2])
    z_out.start()

    def inner(u, v):
        return jnp.sum(u[0] * v[0] + u[1] * v[1] + u[2] * v[2], axis=0, keepdims=True)

    sums = [inner(f, f), inner(f, y), inner(y, y), inner(f, z), inner(y, z)]
    tile = jnp.concatenate(sums + [jnp.zeros((3, BA), F32)], axis=0)
    for shift in (64, 32, 16):
        tile = tile + pltpu.roll(tile, shift, 1)
    row8 = lax.broadcasted_iota(jnp.int32, (8, BA), 0)
    lane8 = lax.broadcasted_iota(jnp.int32, (8, BA), 1)
    packed = jnp.sum(jnp.where(lane8 // 16 == row8, tile, 0.0), axis=0, keepdims=True)

    part[0] = packed
    pl.semaphore_wait(ready, 15)
    xs = [(xx + d) % 4 * 64 for d in range(4)]
    zs = [(zz + d) % 8 * 8 for d in range(8)]
    ys = [(yy + d) % 4 * 2 for d in range(4)]
    cores = (core, 1 - core)
    hops = sorted(
        (-min(dx, 4 - dx) - min(dz, 8 - dz) - min(dy, 4 - dy), -dc, dx, dz, dy)
        for dx in range(4) for dz in range(8) for dy in range(4) for dc in range(2)
    )
    for _, dc, dx, dz, dy in hops[:-1]:
        pltpu.make_async_remote_copy(
            src_ref=part.at[0], dst_ref=others.at[me], send_sem=sum_send.at[0], recv_sem=sum_recv.at[0],
            device_id=(xs[dx] + zs[dz] + ys[dy] + cores[-dc],), device_id_type=MESH,
        ).start()
    others[me] = packed
    pltpu.make_async_copy(others.at[pl.ds(1, 255)], others.at[pl.ds(1, 255)], sum_recv.at[0]).wait()
    pltpu.make_async_copy(others.at[pl.ds(1, 255)], others.at[pl.ds(1, 255)], sum_send.at[0]).wait()
    packed = jnp.sum(others[:, 0, :], axis=0, keepdims=True)

    spread = jnp.broadcast_to(packed, (8, BA))
    first16 = lax.broadcasted_iota(jnp.int32, (8, BA), 1) < 16
    ff, fy, yy_, fz, yz = (
        jnp.where(first16, spread if k == 0 else pltpu.roll(spread, BA - 16 * k, 1), 0.0) for k in range(5)
    )

    def whole(value):
        return jnp.sum(value, axis=1, keepdims=True)

    ff_all = whole(ff)
    step0 = ff_all / whole(fy)
    norm1 = whole((ff - step0 * fy) - step0 * (fy - step0 * yy_))
    beta = norm1 / ff_all
    ry, fq = fy - step0 * yy_, fy - step0 * fz
    rq = fq - step0 * (yy_ - step0 * yz)
    step1 = norm1 / whole(rq + beta * (ry + fq) + beta * beta * fy)
    for target, value in ((step0_ref, step0), (step1_ref, step1), (beta_ref, beta)):
        target[...] = jnp.broadcast_to(value[0:1], (1, BA))
    for copy in (*copies_out, z_out):
        copy.wait()


def kernel(*refs):
    def accumulator(q, rows):
        return pltpu.ACC(q)((rows, 2 * BA), F32)

    def both(x_acc, y_acc, low_acc):
        z_acc = [[(y_acc[q][k][1], low_acc[q][k]) for k in range(2)] for q in range(2)]
        body(x_acc, y_acc, z_acc, *refs)

    pl.run_scoped(
        both,
        [[[accumulator(q, BA) for _ in range(2)] for _ in range(LAG1)] for q in range(2)],
        [[(accumulator(q, 64), accumulator(q, 32)) for _ in range(2)] for q in range(2)],
        [[accumulator(q, 16) for _ in range(2)] for q in range(2)],
    )


PACK = ((0, 3, 4), (3, 1, 5), (4, 5, 2))


def last_step(f_ref, y_ref, z_ref, step0_ref, step1_ref, beta_ref, sol_ref, res_ref):
    step0, step1, beta = (jnp.broadcast_to(ref[...], (BLK, BA)) for ref in (step0_ref, step1_ref, beta_ref))
    for a in range(3):
        first = f_ref[a] - step0 * y_ref[a]
        along = (y_ref[a] - step0 * z_ref[a]) + beta * y_ref[a]
        direction = first + beta * f_ref[a]
        sol_ref[a] = step0 * f_ref[a] + step1 * direction
        res_ref[a] = first - step1 * along


def per_device(coords, force, restraint, neighbors, mask):
    vmem = pl.BlockSpec(memory_space=pltpu.VMEM)
    anywhere = pl.BlockSpec(memory_space=pl.ANY)
    field = jax.ShapeDtypeStruct((3, BLK, BA), F32)
    row = jax.ShapeDtypeStruct((1, BA), F32)
    dma = pltpu.SemaphoreType.DMA
    y, z, step0, step1, beta = pl.pallas_call(
        kernel,
        out_shape=(field, field, row, row, row),
        in_specs=[anywhere] * 5,
        out_specs=(anywhere, anywhere, vmem, vmem, vmem),
        scratch_shapes=[
            pltpu.VMEM((3, BLK, BA), F32),
            pltpu.VMEM((3, BLK, BA), F32),
            pltpu.VMEM((BLK, BA), F32),
            pltpu.VMEM((BLK, NB), jnp.int32),
            pltpu.VMEM((BLK, NB), jnp.int32),
            dma((5,)),
            dma((3,)),
            pltpu.VMEM((3, BLK, BA), F32),
            pltpu.VMEM((2, 3, BLK, BA), F32),
            pltpu.VMEM((2, 3, BLK, BA), F32),
            pltpu.VMEM((2, 3, 8, BA), F32),
            pltpu.VMEM((2, 2, 3, 8, BA), F32),
            pltpu.VMEM((STAGES, 32 * BLK, BA), F32),
            pltpu.VMEM((128, 128), F32),
            pltpu.VMEM((48, 128), F32),
            pltpu.VMEM((48 * BA, 128), BF16),
            pltpu.VMEM((PAIRS, 128, 2 * BA), BF16),
            pltpu.VMEM((64, 48 * BA), BF16),
            pltpu.VMEM((PAIRS, 32 * BA, 2 * BA), BF16),
            pltpu.VMEM((PAIRS, 32 * BA, 2 * BA), F8),
            pltpu.VMEM((PAIRS, 96, 2 * BA), F32),
            pltpu.VMEM((16 * BLK, BA), F32),
            pltpu.VMEM((16 * BLK, BA), F32),
            pltpu.VMEM((2, 6, 8, BA), F32),
            pltpu.VMEM((1, 1, BA), F32),
            pltpu.VMEM((256, 1, BA), F32),
            pltpu.SemaphoreType.REGULAR,
            dma((2,)), dma((2,)), dma((2,)), dma((2,)), dma((2, 2)), dma((2, 2)), dma((2,)), dma((2,)),
        ],
        compiler_params=pltpu.CompilerParams(collective_id=0, has_side_effects=True),
    )(coords.transpose(1, 0, 2), force.transpose(1, 0, 2), restraint, neighbors, mask)
    solution_field, residual = pl.pallas_call(
        last_step,
        out_shape=(field, field),
        in_specs=[vmem] * 6,
        out_specs=(vmem, vmem),
    )(force.transpose(1, 0, 2), y, z, step0, step1, beta)
    return solution_field.transpose(1, 0, 2), residual.transpose(1, 0, 2)


def solution(mesh):
    return jax.shard_map(
        per_device,
        mesh=mesh,
        in_specs=(P(AXIS, None, None), P(AXIS, None, None), P(AXIS, None), P(AXIS, None), P(AXIS, None)),
        out_specs=(P(AXIS, None, None), P(AXIS, None, None)),
        check_vma=False,
    )
```

```python
import functools

import jax
import jax.numpy as jnp
from jax import lax
from jax.experimental import pallas as pl
from jax.experimental.pallas import tpu as pltpu
from jax.sharding import PartitionSpec as P

AXIS = "space"
MESH = pl.DeviceIdType.MESH
BLK = 16
BA = 128
NB = 32
PAIRS = BLK // 2
LAG = 2
LAG1 = LAG + 1
STAGES = 12
F32, BF16, F8 = jnp.float32, jnp.bfloat16, jnp.float8_e4m3fn
SHRINK = 2.0**-8
FAR = 1.5 * 2.0**63
SCALE = SHRINK * SHRINK / BA


def split2(value):
    high = value.astype(BF16).astype(F32)
    return high, value - high


def split3(value):
    high, rest = split2(value)
    middle, low = split2(rest)
    return high, middle, low


def body(
    x_acc, y_acc, z_acc, c_hbm, f_hbm, r_hbm, nb_hbm, mk_hbm, y_hbm, z_hbm, step0_ref, step1_ref, beta_ref,
    c_ref, f_ref, r_ref, nb_ref, mk_ref, in_sem, out_sem, zown,
    halo_c, halo_f, yown, yhalo, stage, enc, far_t, at, bm, feat, wh, wl, yacc, rows_v, rows_s, dmat,
    part, others, ready, c_send, c_recv, f_send, f_recv, y_send, y_recv, sum_send, sum_recv,
):
    me = lax.axis_index(AXIS)
    core, yy, zz, xx = me % 2, (me // 2) % 4, (me // 8) % 8, me // 64
    rank_a, rank_b = zz * 2 + core, xx * 4 + yy

    def member_a(rank):
        return xx * 64 + (rank // 2) * 8 + yy * 2 + rank % 2

    def member_b(rank):
        return (rank // 4) * 64 + zz * 8 + (rank % 4) * 2 + core

    before, after = (me + 255) % 256, (me + 1) % 256
    first, last = me == 0, me == 255

    pairs_in = ((c_hbm, c_ref), (f_hbm, f_ref), (r_hbm, r_ref), (nb_hbm, nb_ref), (mk_hbm, mk_ref))
    loads = [pltpu.make_async_copy(source, target, in_sem.at[k]) for k, (source, target) in enumerate(pairs_in)]
    for load in loads:
        load.start()

    barrier = pltpu.get_barrier_semaphore()
    for target in (before, after):
        pl.semaphore_signal(barrier, inc=1, device_id=(target,), device_id_type=MESH)
    for t in range(1, 16):
        pl.semaphore_signal(barrier, inc=1, device_id=(member_a((rank_a + t) % 16),), device_id_type=MESH)
        pl.semaphore_signal(barrier, inc=1, device_id=(member_b((rank_b + t) % 16),), device_id_type=MESH)

    for load in loads:
        load.wait()

    place = nb_ref[...] - me * BLK + BLK
    enc[...] = jnp.full((128, 128), -1.0, F32)
    enc[32 : 32 + BLK, 0:NB] = jnp.where(mk_ref[...] == 1, place, -1).astype(F32)
    slots = enc[...].T
    window = lax.broadcasted_iota(jnp.int32, (48, 128), 0).astype(F32)
    lane = lax.broadcasted_iota(jnp.int32, (48, 128), 1)
    hit = window == slots[0:1, :]
    for s in range(1, NB):
        hit = jnp.logical_or(hit, window == slots[s : s + 1, :])
    far_t[...] = jnp.where(jnp.logical_or(hit, jnp.logical_or(lane < 32, lane >= 32 + BLK)), 0.0, FAR)

    one = jnp.ones((BLK, BA), F32)

    turn = [0]

    def spread_rows(rows, stride):
        turn[0] = (turn[0] + 1) % STAGES
        target = stage.at[turn[0]]
        for k, row in enumerate(rows):
            target[pl.ds(k, BLK, stride=stride), :] = row
        return target

    def far_side(group, c):
        h, m, l = zip(*(split3(c[a]) for a in range(3)))
        norm = split3(c[0] * c[0] + c[1] * c[1] + c[2] * c[2])
        zero = jnp.zeros((BLK, BA), F32)
        rows = [*h, *h, *h, *m, *m, *l, *norm, one, one, one] + [zero] * 8
        source = spread_rows(rows, 32)

        def fill(e):
            block = group * BLK + e
            tall = jnp.concatenate([source[e * 32 : e * 32 + 32, :], jnp.zeros((96, BA), F32)], axis=0)
            at[block * BA : (block + 1) * BA, :] = (tall.T + far_t[block : block + 1, :]).astype(BF16)

        return fill

    def near_side(c):
        h, m, l = zip(*(split3(c[a]) for a in range(3)))
        norm = split3(1.0 + (c[0] * c[0] + c[1] * c[1] + c[2] * c[2]))
        zero = jnp.zeros((BLK, BA), F32)
        h, m, l = ([-2.0 * SHRINK * v for v in vs] for vs in (h, m, l))
        norm = [SHRINK * v for v in norm]
        shrink = jnp.full((BLK, BA), SHRINK, F32)
        rows = [*h, *m, *l, *h, *m, *h, shrink, shrink, shrink, *norm] + [zero] * 8
        source = spread_rows(rows, 32)
        row = lax.broadcasted_iota(jnp.int32, (96, BA), 0)
        for b in range(BLK):
            lanes = slice((b % 2) * BA, (b % 2 + 1) * BA)
            full = jnp.concatenate([source[b * 32 : b * 32 + 32, :], jnp.where(row == b, 1.0, 0.0)], axis=0)
            bm[b // 2, :, lanes] = full.astype(BF16)

    def store_features(group, values, high_row, low_row):
        highs, lows = zip(*(split2(v) for v in values))
        sources = [(spread_rows(split, 16), row) for split, row in ((highs, high_row), (lows, low_row))]

        def fill(e):
            lanes = slice((group * BLK + e) * BA, (group * BLK + e + 1) * BA)
            for source, row in sources:
                feat[row : row + 16, lanes] = source[e * 16 : e * 16 + 16, :].astype(BF16)

        return fill

    def field_features(group, c, v):
        p = c[0] * v[0] + c[1] * v[1] + c[2] * v[2]
        values = [c[a] * p for a in range(3)] + [p] + [v[b] for b in range(3)]
        values += [c[a] * v[b] for a in range(3) for b in range(3)]
        return store_features(group, values, 16, 0)

    def place_features(group, c):
        zero = jnp.zeros((BLK, BA), F32)
        values = [one, c[0], c[1], c[2], c[0] * c[0], c[1] * c[1], c[2] * c[2]]
        values += [c[0] * c[1], c[0] * c[2], c[1] * c[2]] + [zero] * 6
        return store_features(group, values, 32, 48)

    def fill_all(*fills):
        for e in range(BLK):
            for fill in fills:
                fill(e)

    def tiles_of(p, inside):
        if inside:
            return [((BLK + 2 * k, BLK + 2 * k + 1), k) for k in range(8)]
        low = [(e, e + 1) for e in range(2 * p + 2, BLK, 2)]
        up = [(e, e + 1) for e in range(2 * BLK, 2 * BLK + 2 * p, 2)]
        return [(blocks, 8 + k) for k, blocks in enumerate(low + up + [(2 * p + 1, 2 * BLK + 2 * p)])]

    def lanes_of(rows, blocks):
        i, j = blocks
        if j == i + 1:
            return feat[rows, i * BA : (j + 1) * BA]
        return jnp.concatenate([feat[rows, e * BA : (e + 1) * BA] for e in blocks], axis=1)

    zeros = jnp.zeros((BA, BA), BF16)
    register = [0, 0]

    def push(q, tile):
        register[q] = 1 - register[q]
        pltpu.matmul_push_rhs(tile, staging_register=register[q], mxu_index=q)
        return register[q]

    steps = [(pair, t) for pair in range(PAIRS // 2) for t in range(8)]

    def build(inside, ahead=None, collected=None):
        lists = [tiles_of(p, inside) for p in range(PAIRS)]

        def start(q, i):
            pair, t = steps[i]
            p = 2 * pair + q
            wide = jnp.concatenate([bm[p], jnp.zeros((BA, 2 * BA), BF16)], axis=0)
            staged = push(q, wide)
            for k, e in enumerate(lists[p][t][0]):
                lhs = jnp.concatenate([at[e * BA : (e + 1) * BA, :], zeros], axis=1)
                pltpu.matmul_acc_lhs(x_acc[q][i % LAG1][k], lhs, load_staged_rhs=staged if k == 0 else None)

        def finish(q, i):
            pair, t = steps[i]
            p = 2 * pair + q
            blocks, slot = lists[p][t]
            for k in range(2):
                x = pltpu.matmul_pop(x_acc[q][i % LAG1][k])
                w = 1.0 / (x * x)
                high = w.astype(BF16)
                rows = slice(slot * 2 * BA + k * BA, slot * 2 * BA + (k + 1) * BA)
                wh[p, rows, :] = high
                low = (w - wh[p, rows, :].astype(F32)).astype(F8)
                wl[p, rows, :] = low
            acc_h, acc_l = y_acc[q][pair % 2]
            tile = slice(slot * 2 * BA, (slot + 1) * 2 * BA)
            staged = push(q, wh[p, tile, :])
            pltpu.matmul_acc_lhs(acc_h, lanes_of(slice(0, 64), blocks), load_staged_rhs=staged)
            staged = push(q, wl[p, tile, :])
            pltpu.matmul_acc_lhs(acc_l, lanes_of(slice(16, 48), blocks), load_staged_rhs=staged)

        def collect(pair):
            for q in range(2):
                p = 2 * pair + q
                acc_h, acc_l = y_acc[q][pair % 2]
                total_h, total_l = pltpu.matmul_pop(acc_h), pltpu.matmul_pop(acc_l)
                if inside:
                    yacc[p, 0:64, :] = total_h
                    yacc[p, 64:96, :] = total_l
                    continue
                total_h += yacc[p, 0:64, :]
                total_l += yacc[p, 64:96, :]
                value = total_h[0:16] + total_h[16:32] + total_l[0:16]
                still = total_h[32:48] + total_h[48:64] + total_l[16:32]
                for k in range(2):
                    rows = slice((2 * p + k) * 16, (2 * p + k + 1) * 16)
                    rows_v[rows, :] = value[:, k * BA : (k + 1) * BA]
                    rows_s[rows, :] = still[:, k * BA : (k + 1) * BA]

        for i in range(len(steps) + LAG):
            if ahead is not None:
                ahead(i)
            for q in range(2):
                if i < len(steps):
                    start(q, i)
            for q in range(2):
                if i >= LAG:
                    finish(q, i - LAG)
            if i >= LAG + 9 and (i - LAG - 9) % 8 == 0:
                collect((i - LAG - 9) // 8)
                if collected is not None:
                    collected((i - LAG - 9) // 8)
        collect(PAIRS // 2 - 1)
        if collected is not None:
            collected(PAIRS // 2 - 1)

    def product(phase):
        lists = [tiles_of(p, phase == 0) for p in range(PAIRS)]
        if phase > 0:
            early = [[tile for tile in tiles if all(e % BLK < 8 for e in tile[0])] for tiles in lists]
            lists = early if phase == 1 else [
                [tile for tile in tiles if tile not in first] for tiles, first in zip(lists, early)
            ]

        def collect(pair):
            for q in range(2):
                p = 2 * pair + q
                acc_h, acc_l = z_acc[q][pair % 2]
                total_h, total_l = pltpu.matmul_pop(acc_h), pltpu.matmul_pop(acc_l)
                value = total_h[0:16] + total_h[16:32] + total_l
                if phase > 0:
                    value += yacc[p, 0:16, :]
                if phase < 2:
                    yacc[p, 0:16, :] = value
                    continue
                for k in range(2):
                    rows_v[(2 * p + k) * 16 : (2 * p + k + 1) * 16, :] = value[:, k * BA : (k + 1) * BA]

        count = len(lists[0])
        assert all(len(tiles) == count for tiles in lists)
        for i in range(PAIRS // 2 * count):
            pair, t = i // count, i % count
            for q in range(2):
                p = 2 * pair + q
                blocks, slot = lists[p][t]
                acc_h, acc_l = z_acc[q][pair % 2]
                rows = slice(slot * 2 * BA, (slot + 1) * 2 * BA)
                staged = push(q, wh[p, rows, :])
                pltpu.matmul_acc_lhs(acc_h, lanes_of(slice(0, 32), blocks), load_staged_rhs=staged)
                staged = push(q, wl[p, rows, :])
                pltpu.matmul_acc_lhs(acc_l, lanes_of(slice(16, 32), blocks), load_staged_rhs=staged)
            if i > count and i % count == 1:
                collect(i // count - 1)
        collect(PAIRS // 2 - 1)

    def combine(half, c, v):
        t = [rows_v[pl.ds(k + half * 128, 8, stride=16), :] for k in range(16)]
        cv = c[0] * t[4] + c[1] * t[5] + c[2] * t[6]
        out = []
        for a in range(3):
            gone = t[a] - c[a] * t[3] + c[a] * cv
            gone = gone - (c[0] * t[7 + 3 * a] + c[1] * t[8 + 3 * a] + c[2] * t[9 + 3 * a])
            kept = sum(dmat[half, PACK[a][b]] * v[b] for b in range(3))
            out.append(kept - gone * SCALE)
        return out

    c = [c_ref[a] for a in range(3)]
    f = [f_ref[a] for a in range(3)]
    near_side(c)
    fill_all(far_side(1, c), field_features(1, c, f), place_features(1, c))

    pl.semaphore_wait(barrier, 32)

    def exchange(source, target, send, recv):
        up, down = (
            pltpu.make_async_remote_copy(
                src_ref=source, dst_ref=target.at[k], send_sem=send.at[k], recv_sem=recv.at[k],
                device_id=(neighbour,), device_id_type=MESH,
            )
            for k, neighbour in ((0, after), (1, before))
        )

        @pl.when(jnp.logical_not(last))
        def _():
            up.start()

        @pl.when(jnp.logical_not(first))
        def _():
            down.start()

        @pl.when(first)
        def _():
            target[0] = jnp.zeros(target.shape[1:], F32)

        @pl.when(last)
        def _():
            target[1] = jnp.zeros(target.shape[1:], F32)

        def finish():
            @pl.when(jnp.logical_not(last))
            def _():
                up.wait_send()
                down.wait_recv()

            @pl.when(jnp.logical_not(first))
            def _():
                down.wait_send()
                up.wait_recv()

        return finish

    finish_c = exchange(c_ref, halo_c, c_send, c_recv)
    finish_f = exchange(f_ref, halo_f, f_send, f_recv)
    for t in range(1, 16):
        pl.semaphore_signal(ready, inc=1, device_id=(member_b((rank_b + t) % 16),), device_id_type=MESH)

    build(True)

    finish_c()
    hc = [[halo_c[side, a] for a in range(3)] for side in range(2)]
    far_fill, field_fill = {}, {}

    def open_far(side):
        far_fill[side] = far_side(2 * side, hc[side])

    def open_fields(side):
        hf = [halo_f[side, a] for a in range(3)]
        fills = (field_features(2 * side, hc[side], hf), place_features(2 * side, hc[side]))
        field_fill[side] = lambda e: [fill(e) for fill in fills]

    def fill_blocks(fills, side, *blocks):
        for e in blocks:
            fills[side](e)

    def ahead(i):
        if i == 0:
            open_far(0)
            fill_blocks(far_fill, 0, 2, 3, 4, 5)
        if i == 1:
            fill_blocks(far_fill, 0, 6, 7)
            finish_f()
            open_fields(0)
            fill_blocks(field_fill, 0, 2, 3, 4, 5)
        if i == 2:
            fill_blocks(far_fill, 0, 8, 9)
            fill_blocks(field_fill, 0, 6, 7)
            open_far(1)
        if i == 3:
            fill_blocks(far_fill, 0, 10, 11)
            fill_blocks(field_fill, 0, 8, 9)
            fill_blocks(far_fill, 1, 0, 1, 2)
        if i == 4:
            fill_blocks(far_fill, 0, 12, 13)
            fill_blocks(field_fill, 0, 10, 11)
            fill_blocks(far_fill, 1, 3, 4, 5, 6)
            open_fields(1)
        if i == 5:
            fill_blocks(far_fill, 0, 14, 15, 1)
            fill_blocks(field_fill, 0, 12, 13)
            fill_blocks(far_fill, 1, 7, 8, 9, 10)
            fill_blocks(field_fill, 1, 0, 1, 2, 3)
        if i == 6:
            fill_blocks(far_fill, 1, 11, 12, 13, 14)
            fill_blocks(field_fill, 0, 14, 15, 1)
            fill_blocks(field_fill, 1, 4, 5, 6, 7, 8)
        if i == 7:
            fill_blocks(field_fill, 1, 9, 10, 11, 12, 13, 14)

    finishes, copies_out = [], []

    def first_product(pair):
        if pair % 2 == 0:
            return
        half = pair // 2
        rows = slice(8 * half, 8 * half + 8)
        ch = [c_ref[a, rows] for a in range(3)]
        fh = [f_ref[a, rows] for a in range(3)]
        s = [rows_s[pl.ds(k + half * 128, 8, stride=16), :] for k in range(10)]
        for a, b, k in ((0, 0, 4), (1, 1, 5), (2, 2, 6), (0, 1, 7), (0, 2, 8), (1, 2, 9)):
            entry = (s[k] - ch[a] * s[1 + b] - ch[b] * s[1 + a] + ch[a] * ch[b] * s[0]) * SCALE
            dmat[half, PACK[a][b]] = entry + r_ref[rows] if a == b else entry
        value = combine(half, ch, fh)
        for a in range(3):
            yown[half, a] = value[a]
        finishes.append(exchange(yown.at[half], yhalo.at[half], y_send.at[half], y_recv.at[half]))
        copies_out.append(pltpu.make_async_copy(yown.at[half], y_hbm.at[:, rows], out_sem.at[half]))
        copies_out[-1].start()

    build(False, ahead, first_product)

    y = [jnp.concatenate([yown[0, a], yown[1, a]], axis=0) for a in range(3)]
    fill_all(field_features(1, c, y))
    product(0)
    for half in range(2):
        finishes[half]()
        for side in range(2):
            blank = jnp.zeros((8, BA), F32)
            parts = [[yhalo[half, side, a], blank] for a in range(3)]
            hy = [jnp.concatenate(part if half == 0 else part[::-1], axis=0) for part in parts]
            fill = field_features(2 * side, hc[side], hy)
            for e in range(8 * half, 8 * half + 8):
                fill(e)
        product(1 + half)
    halves = [
        combine(half, [c[a][8 * half : 8 * half + 8] for a in range(3)], [yown[half, a] for a in range(3)])
        for half in range(2)
    ]
    z = [jnp.concatenate([halves[0][a], halves[1][a]], axis=0) for a in range(3)]
    for a in range(3):
        zown[a] = z[a]
    z_out = pltpu.make_async_copy(zown, z_hbm, out_sem.at[2])
    z_out.start()

    def inner(u, v):
        return jnp.sum(u[0] * v[0] + u[1] * v[1] + u[2] * v[2], axis=0, keepdims=True)

    sums = [inner(f, f), inner(f, y), inner(y, y), inner(f, z), inner(y, z)]
    tile = jnp.concatenate(sums + [jnp.zeros((3, BA), F32)], axis=0)
    for shift in (64, 32, 16):
        tile = tile + pltpu.roll(tile, shift, 1)
    row8 = lax.broadcasted_iota(jnp.int32, (8, BA), 0)
    lane8 = lax.broadcasted_iota(jnp.int32, (8, BA), 1)
    packed = jnp.sum(jnp.where(lane8 // 16 == row8, tile, 0.0), axis=0, keepdims=True)

    part[0] = packed
    pl.semaphore_wait(ready, 15)
    xs = [(xx + d) % 4 * 64 for d in range(4)]
    zs = [(zz + d) % 8 * 8 for d in range(8)]
    ys = [(yy + d) % 4 * 2 for d in range(4)]
    cores = (core, 1 - core)
    hops = sorted(
        (-min(dx, 4 - dx) - min(dz, 8 - dz) - min(dy, 4 - dy), -dc, dx, dz, dy)
        for dx in range(4) for dz in range(8) for dy in range(4) for dc in range(2)
    )
    for _, dc, dx, dz, dy in hops[:-1]:
        pltpu.make_async_remote_copy(
            src_ref=part.at[0], dst_ref=others.at[me], send_sem=sum_send.at[0], recv_sem=sum_recv.at[0],
            device_id=(xs[dx] + zs[dz] + ys[dy] + cores[-dc],), device_id_type=MESH,
        ).start()
    others[me] = packed
    pltpu.make_async_copy(others.at[pl.ds(1, 255)], others.at[pl.ds(1, 255)], sum_recv.at[0]).wait()
    pltpu.make_async_copy(others.at[pl.ds(1, 255)], others.at[pl.ds(1, 255)], sum_send.at[0]).wait()
    packed = jnp.sum(others[:, 0, :], axis=0, keepdims=True)

    spread = jnp.broadcast_to(packed, (8, BA))
    first16 = lax.broadcasted_iota(jnp.int32, (8, BA), 1) < 16
    ff, fy, yy_, fz, yz = (
        jnp.where(first16, spread if k == 0 else pltpu.roll(spread, BA - 16 * k, 1), 0.0) for k in range(5)
    )

    def whole(value):
        return jnp.sum(value, axis=1, keepdims=True)

    ff_all = whole(ff)
    step0 = ff_all / whole(fy)
    norm1 = whole((ff - step0 * fy) - step0 * (fy - step0 * yy_))
    beta = norm1 / ff_all
    ry, fq = fy - step0 * yy_, fy - step0 * fz
    rq = fq - step0 * (yy_ - step0 * yz)
    step1 = norm1 / whole(rq + beta * (ry + fq) + beta * beta * fy)
    for target, value in ((step0_ref, step0), (step1_ref, step1), (beta_ref, beta)):
        target[...] = jnp.broadcast_to(value[0:1], (1, BA))
    for copy in (*copies_out, z_out):
        copy.wait()


def kernel(*refs):
    def accumulator(q, rows):
        return pltpu.ACC(q)((rows, 2 * BA), F32)

    def both(x_acc, y_acc, low_acc):
        z_acc = [[(y_acc[q][k][1], low_acc[q][k]) for k in range(2)] for q in range(2)]
        body(x_acc, y_acc, z_acc, *refs)

    pl.run_scoped(
        both,
        [[[accumulator(q, BA) for _ in range(2)] for _ in range(LAG1)] for q in range(2)],
        [[(accumulator(q, 64), accumulator(q, 32)) for _ in range(2)] for q in range(2)],
        [[accumulator(q, 16) for _ in range(2)] for q in range(2)],
    )


PACK = ((0, 3, 4), (3, 1, 5), (4, 5, 2))


def last_step(f_ref, y_ref, z_ref, step0_ref, step1_ref, beta_ref, sol_ref, res_ref):
    step0, step1, beta = (jnp.broadcast_to(ref[...], (BLK, BA)) for ref in (step0_ref, step1_ref, beta_ref))
    for a in range(3):
        first = f_ref[a] - step0 * y_ref[a]
        along = (y_ref[a] - step0 * z_ref[a]) + beta * y_ref[a]
        direction = first + beta * f_ref[a]
        sol_ref[a] = step0 * f_ref[a] + step1 * direction
        res_ref[a] = first - step1 * along


def per_device(coords, force, restraint, neighbors, mask):
    vmem = pl.BlockSpec(memory_space=pltpu.VMEM)
    anywhere = pl.BlockSpec(memory_space=pl.ANY)
    field = jax.ShapeDtypeStruct((3, BLK, BA), F32)
    row = jax.ShapeDtypeStruct((1, BA), F32)
    dma = pltpu.SemaphoreType.DMA
    y, z, step0, step1, beta = pl.pallas_call(
        kernel,
        out_shape=(field, field, row, row, row),
        in_specs=[anywhere] * 5,
        out_specs=(anywhere, anywhere, vmem, vmem, vmem),
        scratch_shapes=[
            pltpu.VMEM((3, BLK, BA), F32),
            pltpu.VMEM((3, BLK, BA), F32),
            pltpu.VMEM((BLK, BA), F32),
            pltpu.VMEM((BLK, NB), jnp.int32),
            pltpu.VMEM((BLK, NB), jnp.int32),
            dma((5,)),
            dma((3,)),
            pltpu.VMEM((3, BLK, BA), F32),
            pltpu.VMEM((2, 3, BLK, BA), F32),
            pltpu.VMEM((2, 3, BLK, BA), F32),
            pltpu.VMEM((2, 3, 8, BA), F32),
            pltpu.VMEM((2, 2, 3, 8, BA), F32),
            pltpu.VMEM((STAGES, 32 * BLK, BA), F32),
            pltpu.VMEM((128, 128), F32),
            pltpu.VMEM((48, 128), F32),
            pltpu.VMEM((48 * BA, 128), BF16),
            pltpu.VMEM((PAIRS, 128, 2 * BA), BF16),
            pltpu.VMEM((64, 48 * BA), BF16),
            pltpu.VMEM((PAIRS, 32 * BA, 2 * BA), BF16),
            pltpu.VMEM((PAIRS, 32 * BA, 2 * BA), F8),
            pltpu.VMEM((PAIRS, 96, 2 * BA), F32),
            pltpu.VMEM((16 * BLK, BA), F32),
            pltpu.VMEM((16 * BLK, BA), F32),
            pltpu.VMEM((2, 6, 8, BA), F32),
            pltpu.VMEM((1, 1, BA), F32),
            pltpu.VMEM((256, 1, BA), F32),
            pltpu.SemaphoreType.REGULAR,
            dma((2,)), dma((2,)), dma((2,)), dma((2,)), dma((2, 2)), dma((2, 2)), dma((2,)), dma((2,)),
        ],
        compiler_params=pltpu.CompilerParams(collective_id=0, has_side_effects=True),
    )(coords.transpose(1, 0, 2), force.transpose(1, 0, 2), restraint, neighbors, mask)
    solution_field, residual = pl.pallas_call(
        last_step,
        out_shape=(field, field),
        in_specs=[vmem] * 6,
        out_specs=(vmem, vmem),
    )(force.transpose(1, 0, 2), y, z, step0, step1, beta)
    return solution_field.transpose(1, 0, 2), residual.transpose(1, 0, 2)


def solution(mesh):
    return jax.shard_map(
        per_device,
        mesh=mesh,
        in_specs=(P(AXIS, None, None), P(AXIS, None, None), P(AXIS, None), P(AXIS, None), P(AXIS, None)),
        out_specs=(P(AXIS, None, None), P(AXIS, None, None)),
        check_vma=False,
    )
```
